32 devices in a mesh: scene: 2 (over y), tile: 4 (over z), half: 2 (over x), band: 2 (over core).
Axes of the slice: x: 2, y: 2, z: 4, core: 2. Of those that a mesh axis runs over, the one named last changes fastest.
Arguments:
- optical: bfloat16 [16, 2, 512, 512], P(('scene', 'tile'), 'band', 'half'), parts along dimension 0, may hold values from -64 to 64
- sar: bfloat16 [2, 8192, 512], P('band', ('scene', 'tile', 'half')), parts along dimension 1, may hold values from -64 to 64
- destination: int32 [128], P('scene'), parts along dimension 0, may hold values from 0 to 63, as said below
- peaks: int32 [16, 2, 8], P(('scene', 'tile', 'band')), parts along dimension 0, may hold values from 0 to 511
Outputs:
- surface: float32 [16, 512, 512], P(('scene', 'tile', 'band'), 'half'), parts along dimension 0
- peak_values: float32 [16, 8], P(('scene', 'tile', 'band')), parts along dimension 0
The draws below stay inside these ranges and needn't reach their ends.
There are 2 independent parts, one for each index of `scene`. The reference program is written for one: setup_inputs(seed, part) draws one part's arguments, and reference() takes and returns one part's arrays. A program takes and returns all parts, laid end to end along the dimension named above; each array names one. Nothing has to cross between parts.
Inputs may be any that keep to these rules, and one draw needn't show every extreme that they name: destination holds every block position 0 to 63 once; the 8 blocks that start at each multiple of 8 are sent one into each run of 8 positions that starts at a multiple of 8.
All inputs are finite; a program needn't handle non-finite values.
Results may differ from the reference program's by a relative error of at most 0.014.
Values may be sent and summed in bfloat16 or wider, within the bound.
No kernel may reach another device: no remote copies, remote signals or barrier semaphores. Data moves between devices by JAX's collectives and lax.ppermute only.
A program may use at most 64 MiB of HBM per device.

```python
import math
import jax
import jax.numpy as jnp
from jax import lax

PATCH_SIZE = 512
BAND_COUNT = 2
PATCH_DEV = 2
PEAK_COUNT = 8
PATCHES = 8
GROUP_DEVICES = 8
BLOCK_LINES = 64
BLOCKS = 64
SLANT_LINES = 4096
N_TILE = 4
N_HALF = 2


def one_order(subkey):
    return jax.random.permutation(subkey, GROUP_DEVICES).astype(jnp.int32)


def draw_destination(key, part):
    subkeys = jax.random.split(jax.random.fold_in(key, 7), 2)
    sending = jax.vmap(one_order)(jax.random.split(subkeys[0], GROUP_DEVICES))
    slotting = jax.vmap(one_order)(jax.random.split(subkeys[1], GROUP_DEVICES))
    senders = jnp.arange(GROUP_DEVICES, dtype=jnp.int32)[:, None]
    slot_index = slotting[sending, senders]
    return (sending * GROUP_DEVICES + slot_index).reshape(BLOCKS).astype(jnp.int32)


def draw_optical(key, part):
    full_shape = (PATCHES, BAND_COUNT, PATCH_SIZE, PATCH_SIZE)
    line_frac = jnp.arange(PATCH_SIZE, dtype=jnp.float32)[:, None] / (PATCH_SIZE - 1)
    subkeys = jax.random.split(jax.random.fold_in(key, 3), 1)
    noise_draw = jnp.clip(jax.random.normal(subkeys[0], full_shape, jnp.float32), -5.0, 5.0)
    values = noise_draw * jnp.exp(math.log(3.0) * line_frac - 0.5 * math.log(3.0))
    return values.astype(jnp.bfloat16)


def draw_sar(key, part):
    full_shape = (BAND_COUNT, SLANT_LINES, PATCH_SIZE)
    line_frac = jnp.arange(SLANT_LINES, dtype=jnp.float32)[:, None] / (SLANT_LINES - 1)
    subkeys = jax.random.split(jax.random.fold_in(key, 5), 1)
    noise_draw = jnp.clip(jax.random.normal(subkeys[0], full_shape, jnp.float32), -5.0, 5.0)
    values = noise_draw * jnp.exp(math.log(3.0) * line_frac - 0.5 * math.log(3.0))
    return values.astype(jnp.bfloat16)


def place_ends(entries, own_key, low, high):
    index_at = [jax.random.randint(jax.random.fold_in(own_key, axis), (), 0, length) for axis, length in enumerate(entries.shape)]
    longest = entries.shape.index(max(entries.shape))
    neighbour = index_at[:longest] + [(index_at[longest] + 1) % entries.shape[longest]] + index_at[longest + 1:]
    return entries.at[tuple(index_at)].set(low).at[tuple(neighbour)].set(high)


def setup_inputs(seed: int = 0, part: int = 0) -> dict:
    key_list = jax.random.split(jax.random.key(seed), 5)
    part_splits = jax.random.split(jax.random.fold_in(key_list[4], part), 5)
    optical = draw_optical(jax.random.fold_in(jax.random.fold_in(key_list[4], part), 71), part)
    sar = draw_sar(jax.random.fold_in(jax.random.fold_in(key_list[4], part), 71), part)
    destination = draw_destination(jax.random.fold_in(jax.random.fold_in(key_list[4], part), 71), part)
    peaks = place_ends(jax.random.randint(part_splits[3], (PATCHES, 2, PEAK_COUNT), 0, PATCH_SIZE), jax.random.fold_in(part_splits[3], 1), 0, PATCH_SIZE - 1).astype(jnp.int32)
    return dict(optical=optical, sar=sar, destination=destination, peaks=peaks)


EPSILON = 1e-06

def column_pair(samples):
    spectrum = jnp.fft.fft(samples.astype(jnp.float32), axis=-1)
    return (jnp.real(spectrum).astype(jnp.bfloat16), jnp.imag(spectrum).astype(jnp.bfloat16))

def line_spectrum(samples):
    real_part, imag_part = column_pair(samples)
    joined = real_part.astype(jnp.float32) + 1j * imag_part.astype(jnp.float32)
    spectrum = jnp.fft.fft(joined, axis=-2)
    return spectrum.at[..., 0, 0].set(0.0)

def band_energy(samples):
    values = samples.astype(jnp.float32)
    total_sums = lax.optimization_barrier(jnp.sum(values, axis=(2, 3)))
    squares = lax.optimization_barrier(jnp.sum(values * values, axis=(2, 3)))
    pixel_count = PATCH_SIZE * PATCH_SIZE
    centered = squares - total_sums * total_sums / pixel_count
    return lax.optimization_barrier(jnp.sum(centered, axis=1)) / (BAND_COUNT * pixel_count)

def reference(optical, sar, destination, peaks):
    blocks = sar.reshape(BAND_COUNT, BLOCKS, BLOCK_LINES, PATCH_SIZE)
    placed = jnp.zeros_like(blocks).at[:, destination].set(blocks)
    sar_map = placed.reshape(BAND_COUNT, N_TILE, N_HALF, PATCH_DEV, PATCH_SIZE // N_HALF, PATCH_SIZE)
    sar_map = jnp.transpose(sar_map, (1, 3, 0, 2, 4, 5)).reshape(PATCHES, BAND_COUNT, PATCH_SIZE, PATCH_SIZE)
    opt_spec = line_spectrum(optical)
    sar_spec = line_spectrum(sar_map)
    opt_energy = band_energy(optical)
    sar_energy = band_energy(sar_map)
    cross_sum = lax.optimization_barrier(jnp.sum(jnp.conj(opt_spec) * sar_spec, axis=1))
    correlation = jnp.real(jnp.fft.ifft2(cross_sum, axes=(-2, -1)))
    pixel_count = PATCH_SIZE * PATCH_SIZE
    norm_scale = lax.rsqrt(BAND_COUNT * pixel_count * (opt_energy + EPSILON) * (sar_energy + EPSILON))
    surface = (correlation * norm_scale[:, None, None]).astype(jnp.float32)
    flattened = surface.reshape(PATCHES, pixel_count)
    spots = (peaks[:, 0, :] * PATCH_SIZE + peaks[:, 1, :]).astype(jnp.int32)
    peak_values = jnp.take_along_axis(flattened, spots, axis=1)
    return (surface, peak_values)
```

```python
import math

import jax
import jax.numpy as jnp
import numpy as np
from jax import lax
from jax.experimental import pallas as pl
from jax.experimental.pallas import tpu as pltpu
from jax.sharding import PartitionSpec as P

EPSILON = 1e-06
f32 = jnp.float32
bf16 = jnp.bfloat16


def packed_table(extent, groups):
    width = extent // 2 // groups
    places = np.arange(extent)
    phases = np.outer(places, np.arange(extent // 2)) % extent
    angles = phases * (2.0 * math.pi / extent)
    cosines = np.cos(angles)
    sines = -np.sin(angles)
    sines[:, 0] = 1.0 - 2.0 * (places % 2)
    table = np.stack(
        [cosines.reshape(extent, groups, width), sines.reshape(extent, groups, width)], axis=2
    ).reshape(extent, extent)
    return table.astype(np.float32)


def table_pair(table):
    upper = table.astype(bf16)
    lower = (table - upper.astype(np.float32)).astype(bf16)
    return (jnp.asarray(upper), jnp.asarray(lower))


def dot(left, right):
    return jnp.dot(left, right, preferred_element_type=f32)


def three_parts(value):
    upper = value.astype(bf16)
    rest = value - upper.astype(f32)
    middle = rest.astype(bf16)
    lower = (rest - middle.astype(f32)).astype(bf16)
    return [upper.astype(f32), middle.astype(f32), lower.astype(f32)]


def stat_rows(values, lanes):
    values = values.astype(f32)
    sums = jnp.sum(values, axis=0, keepdims=True)
    squares = jnp.sum(values * values, axis=0, keepdims=True)
    rows = []
    for row in (sums, squares):
        folded = row[:, :lanes]
        for at in range(lanes, row.shape[1], lanes):
            folded = folded + row[:, at : at + lanes]
        rows += three_parts(folded)
    return rows


def pad_tile(rows, count, lanes):
    index = lax.broadcasted_iota(jnp.int32, (count, lanes), 0)
    tile = jnp.zeros((count, lanes), f32)
    for at, row in enumerate(rows):
        tile = jnp.where(index == at, row, tile)
    return tile.astype(bf16)


def round_up(value, step):
    return (value + step - 1) // step * step


def swap_halves(value):
    width = value.shape[1] // 2
    if value.shape[1] == 128:
        return pltpu.roll(value, width, 1)
    return jnp.concatenate([value[:, width:], value[:, :width]], axis=1)


def vmem():
    return pl.BlockSpec(memory_space=pltpu.VMEM)


def smem():
    return pl.BlockSpec(memory_space=pltpu.SMEM)


def local(optical, sar, destination, peaks):
    tile_count = lax.axis_size("tile")
    half_count = lax.axis_size("half")
    band_count = lax.axis_size("band")
    group_size = tile_count * half_count
    patch_dev, local_bands, quarter, extent = optical.shape
    assert local_bands == 1
    block_lines = sar.shape[1] // group_size
    pixel_count = extent * extent
    kept = patch_dev // band_count
    peak_count = peaks.shape[2]
    quads = half_count * band_count
    lanes = extent // quads
    width = lanes // 2
    patch_slots = quarter // block_lines
    direct = block_lines % 16 == 0
    table = packed_table(extent, quads)
    t_upper, t_lower = table_pair(table)
    r_upper, r_lower = table_pair(np.ascontiguousarray(table.T))
    tile_at = lax.axis_index("tile")
    half_at = lax.axis_index("half")
    band_at = lax.axis_index("band")
    device_at = lax.axis_index(("tile", "half"))
    quad_at = half_at * band_count + band_at
    params = pltpu.CompilerParams(vmem_limit_bytes=48 * 1024 * 1024)

    peak_list = [peaks]
    for step in range(1, band_count):
        route = [((at + step) % band_count, at) for at in range(band_count)]
        peak_list.append(lax.ppermute(peaks, "band", route))
    peak_lines = jnp.stack([entry[:, 0, :] for entry in peak_list])

    main_rows = half_count * block_lines
    sar_pad = round_up(6 * half_count, 16)
    sar_rows = main_rows + sar_pad

    def sar_kernel(at_ref, dest_ref, sar_ref, up_ref, low_ref, out_ref, order_ref):
        if direct:
            for n in range(group_size):
                order_ref[dest_ref[at_ref[0] * group_size + n] // group_size] = n
            blocks = [
                sar_ref[0, pl.ds(pl.multiple_of(order_ref[g] * block_lines, block_lines), block_lines), :]
                for g in range(group_size)
            ]
            values = jnp.concatenate(blocks, axis=0)
        else:
            values = sar_ref[0]
        spectrum = (dot(values, up_ref[...]) + dot(values, low_ref[...])).astype(bf16)
        for t in range(tile_count):
            rows = []
            for h in range(half_count):
                start = (t * half_count + h) * block_lines
                rows += stat_rows(values[start : start + block_lines], lanes)
            pad = pad_tile(rows, sar_pad, lanes)
            lines = spectrum[t * main_rows : (t + 1) * main_rows]
            for q in range(quads):
                out_ref[t * quads + q, :main_rows, :] = lines[:, q * lanes : (q + 1) * lanes]
                out_ref[t * quads + q, main_rows:, :] = pad

    sar_in = sar
    dest_in = destination
    if not direct:
        own_blocks = lax.dynamic_slice_in_dim(destination, device_at * group_size, group_size)
        order = jnp.argsort(own_blocks // group_size)
        sar_in = jnp.take(
            sar.reshape(group_size, block_lines, extent), order, axis=0
        ).reshape(sar.shape)
        dest_in = own_blocks[:1]
    sar_out = pl.pallas_call(
        sar_kernel,
        out_shape=jax.ShapeDtypeStruct((tile_count * quads, sar_rows, lanes), bf16),
        in_specs=[smem(), smem(), vmem(), vmem(), vmem()],
        out_specs=vmem(),
        scratch_shapes=[pltpu.SMEM((group_size,), jnp.int32)],
        compiler_params=params,
        name="sar_columns",
    )(device_at.reshape(1), dest_in, sar_in, t_upper, t_lower)
    sar_got = lax.all_to_all(
        sar_out, ("tile", "half", "band"), split_axis=0, concat_axis=0, tiled=True
    )

    opt_main = patch_dev * quarter
    opt_pad = round_up(6 * patch_dev, 16)

    def opt_kernel(opt_ref, up_ref, low_ref, out_ref):
        rows = []
        for p in range(patch_dev):
            values = opt_ref[p, 0]
            rows += stat_rows(values, lanes)
            spectrum = (dot(values, up_ref[...]) + dot(values, low_ref[...])).astype(bf16)
            for q in range(quads):
                out_ref[q, p * quarter : (p + 1) * quarter, :] = spectrum[:, q * lanes : (q + 1) * lanes]
        pad = pad_tile(rows, opt_pad, lanes)
        for q in range(quads):
            out_ref[q, opt_main:, :] = pad

    opt_out = pl.pallas_call(
        opt_kernel,
        out_shape=jax.ShapeDtypeStruct((quads, opt_main + opt_pad, lanes), bf16),
        in_specs=[vmem(), vmem(), vmem()],
        out_specs=vmem(),
        compiler_params=params,
        name="opt_columns",
    )(optical, t_upper, t_lower)
    opt_got = lax.all_to_all(opt_out, ("half", "band"), split_axis=0, concat_axis=0, tiled=True)

    slots = half_count * group_size
    lag_rows = quarter + 2 * peak_count
    columns = patch_dev * band_count * lanes

    def middle_kernel(
        at_ref, dest_ref, peak_ref, sar_ref, stat_ref, opt_ref,
        up_ref, low_ref, tup_ref, tlow_ref, out_ref,
        slot_ref, sar_x, opt_x, sar_y, opt_y, freq, lag,
    ):
        base = at_ref[0] * slots
        if direct:
            def place(n, carry):
                offset = dest_ref[n] - base
                inside = (offset >= 0) & (offset < slots)
                slot_ref[jnp.where(inside, offset, slots)] = n // group_size
                return carry

            lax.fori_loop(0, group_size * group_size, place, 0)
        opt_stat = [opt_ref[q, opt_main:, :].astype(f32) for q in range(quads)]
        opt_index = lax.broadcasted_iota(jnp.int32, (opt_pad, lanes), 0)
        sar_index = lax.broadcasted_iota(jnp.int32, (sar_pad, lanes), 0)
        scales = []
        for p in range(patch_dev):
            energies = [jnp.zeros((1, 1), f32), jnp.zeros((1, 1), f32)]
            for b in range(band_count):
                at = (p * band_count + b) * lanes
                acc = opt_stat[b]
                for h in range(1, half_count):
                    acc = acc + opt_stat[h * band_count + b]
                moments = []
                for kind in range(2):
                    first = p * 6 + kind * 3
                    hit = (opt_index >= first) & (opt_index < first + 3)
                    moments.append(jnp.sum(jnp.where(hit, acc, 0.0), keepdims=True))
                energies[0] = energies[0] + (moments[1] - moments[0] * moments[0] / pixel_count)
                for h in range(half_count):
                    opt_x[h * quarter : (h + 1) * quarter, at : at + lanes] = opt_ref[
                        h * band_count + b, p * quarter : (p + 1) * quarter, :
                    ]
                if direct:
                    moments = [jnp.zeros((1, 1), f32), jnp.zeros((1, 1), f32)]
                    for h in range(half_count):
                        acc = jnp.zeros((sar_pad, lanes), f32)
                        for s in range(patch_slots):
                            source = slot_ref[h * group_size + p * patch_slots + s] * band_count + b
                            line = h * quarter + s * block_lines
                            sar_x[line : line + block_lines, at : at + lanes] = sar_ref[
                                source, h * block_lines : (h + 1) * block_lines, :
                            ]
                            acc = acc + sar_ref[source, main_rows:, :].astype(f32)
                        for kind in range(2):
                            first = h * 6 + kind * 3
                            hit = (sar_index >= first) & (sar_index < first + 3)
                            moments[kind] = moments[kind] + jnp.sum(
                                jnp.where(hit, acc, 0.0), keepdims=True
                            )
                else:
                    sar_x[:, at : at + lanes] = sar_ref[b, p]
                    moments = [jnp.full((1, 1), stat_ref[(p * band_count + b) * 2 + kind]) for kind in range(2)]
                energies[1] = energies[1] + (moments[1] - moments[0] * moments[0] / pixel_count)
            energies = [entry / (band_count * pixel_count) for entry in energies]
            scales.append(
                lax.rsqrt(band_count * pixel_count * (energies[0] + EPSILON) * (energies[1] + EPSILON))
                / pixel_count
            )
        opt_y[...] = dot(up_ref[...], opt_x[...]) + dot(low_ref[...], opt_x[...])
        sar_y[...] = dot(up_ref[...], sar_x[...]) + dot(low_ref[...], sar_x[...])
        lane = lax.broadcasted_iota(jnp.int32, (width, lanes), 1)
        row = lax.broadcasted_iota(jnp.int32, (width, lanes), 0)
        left = lane < width
        real_lane = ((lane == 0) | (lane == width)) & (at_ref[2] == 0)
        weight = jnp.where(real_lane, 2.0, 4.0).astype(f32)
        for p in range(patch_dev):
            for g in range(quads):
                cos_rows = slice(g * lanes, g * lanes + width)
                sin_rows = slice(g * lanes + width, (g + 1) * lanes)
                aa = bb = ab = ra = rb = rab = 0.0
                for b in range(band_count):
                    at = (p * band_count + b) * lanes
                    cut = slice(at, at + lanes)
                    ao, bo = opt_y[cos_rows, cut], opt_y[sin_rows, cut]
                    as_, bs = sar_y[cos_rows, cut], sar_y[sin_rows, cut]
                    ras, rbs = swap_halves(as_), swap_halves(bs)
                    aa = aa + ao * as_
                    bb = bb + bo * bs
                    ab = ab + (ao * bs - bo * as_)
                    ra = ra + ao * ras
                    rb = rb + bo * rbs
                    rab = rab + (ao * rbs - bo * ras)
                even, even_turned = aa + bb, ra + rb
                odd, odd_turned = ab, rab
                scale = weight * scales[p]
                if g == 0:
                    first = row == 0
                    even = jnp.where(first, aa, even)
                    even_turned = jnp.where(first, ra, even_turned)
                    odd = jnp.where(first, bb, odd)
                    odd_turned = jnp.where(first, rb, odd_turned)
                    scale = jnp.where(first, 0.5 * scale, scale)

                def combine(plain, turned):
                    pair = jnp.where(
                        left, plain + swap_halves(plain), swap_halves(turned) - turned
                    )
                    return jnp.where(real_lane, plain, pair) * scale

                even = combine(even, even_turned)
                odd = combine(odd, odd_turned)
                if g == 0:
                    even = jnp.where(first & real_lane & (lane == 0), 0.0, even)
                freq[cos_rows, p * lanes : (p + 1) * lanes] = even
                freq[sin_rows, p * lanes : (p + 1) * lanes] = odd
        upper = freq[...].astype(bf16)
        lower = (freq[...] - upper.astype(f32)).astype(bf16)
        back = dot(tup_ref[...], upper) + dot(tup_ref[...], lower) + dot(tlow_ref[...], upper)
        for p in range(patch_dev):
            lag[p] = back[:, p * lanes : (p + 1) * lanes]
        for b in range(band_count):
            turn = (b - at_ref[1] + band_count) % band_count
            for k in range(kept):
                p = b * kept + k
                picked = jnp.concatenate(
                    [lag[p, pl.ds(peak_ref[turn, k, j], 1), :] for j in range(peak_count)], axis=0
                )
                upper = picked.astype(bf16).astype(f32)
                picked = jnp.concatenate([upper, picked - upper], axis=0).astype(bf16)
                for h in range(half_count):
                    out_ref[h * band_count + b, k, :quarter, :] = lag[
                        p, h * quarter : (h + 1) * quarter, :
                    ].astype(bf16)
                    out_ref[h * band_count + b, k, quarter:, :] = picked

    sar_mid = sar_got
    sar_stats = jnp.zeros((2,), f32)
    dest_mid = destination
    if not direct:
        inverse = (
            jnp.zeros_like(destination)
            .at[destination]
            .set(jnp.arange(destination.shape[0], dtype=jnp.int32))
        )
        sources = (
            lax.dynamic_slice_in_dim(inverse, tile_at * slots, slots).reshape(half_count, group_size)
            // group_size
        )
        halves = jnp.arange(half_count, dtype=jnp.int32)[:, None]
        got = sar_got.reshape(group_size, band_count, sar_rows, lanes)
        lines = got[:, :, :main_rows].reshape(
            group_size, band_count, half_count, block_lines, lanes
        )
        lines = jnp.transpose(lines, (0, 2, 1, 3, 4))[sources, halves]
        sar_mid = jnp.transpose(
            lines.reshape(half_count, patch_dev, patch_slots, band_count, block_lines, lanes),
            (3, 1, 0, 2, 4, 5),
        ).reshape(band_count, patch_dev, extent, lanes)
        stats = got[:, :, main_rows : main_rows + 6 * half_count].astype(f32)
        stats = stats.reshape(group_size, band_count, half_count, 2, 3 * lanes).sum(axis=-1)
        stats = jnp.transpose(stats, (0, 2, 1, 3))[sources, halves]
        sar_stats = jnp.transpose(
            stats.reshape(half_count, patch_dev, patch_slots, band_count, 2).sum(axis=(0, 2)),
            (0, 1, 2),
        ).reshape(-1)
        dest_mid = destination[:1]

    lag_out = pl.pallas_call(
        middle_kernel,
        out_shape=jax.ShapeDtypeStruct((quads, kept, lag_rows, lanes), bf16),
        in_specs=[smem(), smem(), smem(), vmem(), smem()] + [vmem()] * 5,
        out_specs=vmem(),
        scratch_shapes=[
            pltpu.SMEM((slots + 1 if direct else 1,), jnp.int32),
            pltpu.VMEM((extent, columns), bf16),
            pltpu.VMEM((extent, columns), bf16),
            pltpu.VMEM((extent, columns), f32),
            pltpu.VMEM((extent, columns), f32),
            pltpu.VMEM((extent, patch_dev * lanes), f32),
            pltpu.VMEM((patch_dev, extent, lanes), f32),
        ],
        compiler_params=params,
        name="lines_and_cross",
    )(
        jnp.stack([tile_at, band_at, quad_at]), dest_mid, peak_lines, sar_mid, sar_stats, opt_got,
        r_upper, r_lower, t_upper, t_lower,
    )
    lag_got = lax.all_to_all(lag_out, ("half", "band"), split_axis=0, concat_axis=0, tiled=True)

    def last_kernel(peak_ref, lag_ref, up_ref, low_ref, out_ref, value_ref):
        for k in range(kept):
            values = jnp.concatenate([lag_ref[q, k] for q in range(quads)], axis=1)
            result = dot(values, up_ref[...]) + dot(values, low_ref[...])
            out_ref[k] = result[:quarter]
            picked = result[quarter : quarter + peak_count] + result[quarter + peak_count :]
            lane = lax.broadcasted_iota(jnp.int32, (peak_count, extent), 1)
            row = lax.broadcasted_iota(jnp.int32, (peak_count, extent), 0)
            wanted = jnp.zeros((peak_count, extent), jnp.int32)
            for j in range(peak_count):
                wanted = jnp.where(row == j, peak_ref[k, 1, j], wanted)
            chosen = jnp.sum(jnp.where(lane == wanted, picked, 0.0), axis=1, keepdims=True)
            line = jnp.sum(jnp.where(lane == row, chosen, 0.0), axis=0, keepdims=True)
            value_ref[k : k + 1, :] = line[:, :peak_count]

    surface, peak_values = pl.pallas_call(
        last_kernel,
        out_shape=(
            jax.ShapeDtypeStruct((kept, quarter, extent), f32),
            jax.ShapeDtypeStruct((kept, peak_count), f32),
        ),
        in_specs=[smem(), vmem(), vmem(), vmem()],
        out_specs=(vmem(), vmem()),
        compiler_params=params,
        name="columns_back",
    )(peaks, lag_got, r_upper, r_lower)
    return (surface, peak_values)


def solution(mesh):
    in_specs = (
        P(("scene", "tile"), "band", "half", None),
        P("band", ("scene", "tile", "half"), None),
        P("scene"),
        P(("scene", "tile", "band"), None, None),
    )
    out_specs = (P(("scene", "tile", "band"), "half", None), P(("scene", "tile", "band"), None))
    return jax.shard_map(local, mesh=mesh, in_specs=in_specs, out_specs=out_specs, check_vma=False)
```

```python
import math

import jax
import jax.numpy as jnp
import numpy as np
from jax import lax
from jax.experimental import pallas as pl
from jax.experimental.pallas import tpu as pltpu
from jax.sharding import PartitionSpec as P

EPSILON = 1e-06
f32 = jnp.float32
bf16 = jnp.bfloat16


def packed_table(extent, groups):
    width = extent // 2 // groups
    places = np.arange(extent)
    phases = np.outer(places, np.arange(extent // 2)) % extent
    angles = phases * (2.0 * math.pi / extent)
    cosines = np.cos(angles)
    sines = -np.sin(angles)
    sines[:, 0] = 1.0 - 2.0 * (places % 2)
    table = np.stack(
        [cosines.reshape(extent, groups, width), sines.reshape(extent, groups, width)], axis=2
    ).reshape(extent, extent)
    return table.astype(np.float32)


def table_pair(table):
    upper = table.astype(bf16)
    lower = (table - upper.astype(np.float32)).astype(bf16)
    return (jnp.asarray(upper), jnp.asarray(lower))


def dot(left, right):
    return jnp.dot(left, right, preferred_element_type=f32)


def three_parts(value):
    upper = value.astype(bf16)
    rest = value - upper.astype(f32)
    middle = rest.astype(bf16)
    lower = (rest - middle.astype(f32)).astype(bf16)
    return [upper.astype(f32), middle.astype(f32), lower.astype(f32)]


def stat_rows(values, lanes):
    values = values.astype(f32)
    sums = jnp.sum(values, axis=0, keepdims=True)
    squares = jnp.sum(values * values, axis=0, keepdims=True)
    rows = []
    for row in (sums, squares):
        folded = row[:, :lanes]
        for at in range(lanes, row.shape[1], lanes):
            folded = folded + row[:, at : at + lanes]
        rows += three_parts(folded)
    return rows


def pad_tile(rows, count, lanes):
    index = lax.broadcasted_iota(jnp.int32, (count, lanes), 0)
    tile = jnp.zeros((count, lanes), f32)
    for at, row in enumerate(rows):
        tile = jnp.where(index == at, row, tile)
    return tile.astype(bf16)


def round_up(value, step):
    return (value + step - 1) // step * step


def swap_halves(value):
    width = value.shape[1] // 2
    if value.shape[1] == 128:
        return pltpu.roll(value, width, 1)
    return jnp.concatenate([value[:, width:], value[:, :width]], axis=1)


def exchange(parcels, axes):
    count = len(parcels)
    got = [parcels[0]] + [None] * (count - 1)
    for d in reversed(range(1, count)):
        got[d] = lax.ppermute(parcels[d], axes, [(at, at ^ d) for at in range(count)])
    return got


def vmem():
    return pl.BlockSpec(memory_space=pltpu.VMEM)


def smem():
    return pl.BlockSpec(memory_space=pltpu.SMEM)


def local(optical, sar, destination, peaks):
    tile_count = lax.axis_size("tile")
    half_count = lax.axis_size("half")
    band_count = lax.axis_size("band")
    group_size = tile_count * half_count
    patch_dev, local_bands, quarter, extent = optical.shape
    assert local_bands == 1
    block_lines = sar.shape[1] // group_size
    pixel_count = extent * extent
    kept = patch_dev // band_count
    peak_count = peaks.shape[2]
    quads = half_count * band_count
    lanes = extent // quads
    width = lanes // 2
    patch_slots = quarter // block_lines
    members = tile_count * quads
    direct = block_lines % 16 == 0 and members <= 16 and members & (members - 1) == 0
    assert quads & (quads - 1) == 0
    table = packed_table(extent, quads)
    t_upper, t_lower = table_pair(table)
    r_upper, r_lower = table_pair(np.ascontiguousarray(table.T))
    tile_at = lax.axis_index("tile")
    half_at = lax.axis_index("half")
    band_at = lax.axis_index("band")
    device_at = lax.axis_index(("tile", "half"))
    quad_at = half_at * band_count + band_at
    member_at = tile_at * quads + quad_at
    places = jnp.stack([tile_at, band_at, quad_at, member_at])
    params = pltpu.CompilerParams(vmem_limit_bytes=48 * 1024 * 1024)

    peak_list = [peaks]
    for step in range(1, band_count):
        route = [((at + step) % band_count, at) for at in range(band_count)]
        peak_list.append(lax.ppermute(peaks, "band", route))
    peak_lines = jnp.stack([entry[:, 0, :] for entry in peak_list])

    main_rows = half_count * block_lines
    sar_pad = round_up(6 * half_count, 16)
    sar_rows = main_rows + sar_pad

    def sar_kernel(at_ref, dest_ref, sar_ref, up_ref, low_ref, *rest):
        out_refs = rest[:-3]
        order_ref, spec, pads = rest[-3:]
        if direct:
            for n in range(group_size):
                order_ref[dest_ref[at_ref[0] * group_size + n] // group_size] = n
            blocks = [
                sar_ref[0, pl.ds(pl.multiple_of(order_ref[g] * block_lines, block_lines), block_lines), :]
                for g in range(group_size)
            ]
            values = jnp.concatenate(blocks, axis=0)
        else:
            values = sar_ref[0]
        spectrum = (dot(values, up_ref[...]) + dot(values, low_ref[...])).astype(bf16)
        if direct:
            for q in range(quads):
                spec[q] = spectrum[:, q * lanes : (q + 1) * lanes]
        for t in range(tile_count):
            rows = []
            for h in range(half_count):
                start = (t * half_count + h) * block_lines
                rows += stat_rows(values[start : start + block_lines], lanes)
            pad = pad_tile(rows, sar_pad, lanes)
            if direct:
                pads[t] = pad
                continue
            lines = spectrum[t * main_rows : (t + 1) * main_rows]
            for q in range(quads):
                out_refs[0][t * quads + q, :main_rows, :] = lines[:, q * lanes : (q + 1) * lanes]
                out_refs[0][t * quads + q, main_rows:, :] = pad
        if direct:
            for d in range(members):
                to = at_ref[1] ^ d
                t = to // quads
                start = pl.multiple_of(t * main_rows, main_rows)
                out_refs[d][:main_rows, :] = spec[to % quads, pl.ds(start, main_rows), :]
                out_refs[d][main_rows:, :] = pads[t]

    sar_in = sar
    dest_in = destination
    if not direct:
        own_blocks = lax.dynamic_slice_in_dim(destination, device_at * group_size, group_size)
        order = jnp.argsort(own_blocks // group_size)
        sar_in = jnp.take(
            sar.reshape(group_size, block_lines, extent), order, axis=0
        ).reshape(sar.shape)
        dest_in = own_blocks[:1]
    parcel_count = members if direct else 1
    parcel_shape = (sar_rows, lanes) if direct else (members, sar_rows, lanes)
    sar_out = pl.pallas_call(
        sar_kernel,
        out_shape=[jax.ShapeDtypeStruct(parcel_shape, bf16)] * parcel_count,
        in_specs=[smem(), smem(), vmem(), vmem(), vmem()],
        out_specs=[vmem()] * parcel_count,
        scratch_shapes=[
            pltpu.SMEM((group_size,), jnp.int32),
            pltpu.VMEM((quads, group_size * block_lines, lanes), bf16),
            pltpu.VMEM((tile_count, sar_pad, lanes), bf16),
        ],
        compiler_params=params,
        name="sar_columns",
    )(jnp.stack([device_at, member_at]), dest_in, sar_in, t_upper, t_lower)
    if direct:
        sar_got = exchange(sar_out, ("tile", "half", "band"))
    else:
        sar_got = lax.all_to_all(
            sar_out[0], ("tile", "half", "band"), split_axis=0, concat_axis=0, tiled=True
        )

    opt_main = patch_dev * quarter
    opt_pad = round_up(6 * patch_dev, 16)

    def opt_kernel(at_ref, opt_ref, up_ref, low_ref, *rest):
        out_refs, spec = rest[:-1], rest[-1]
        rows = []
        for p in range(patch_dev):
            values = opt_ref[p, 0]
            rows += stat_rows(values, lanes)
            spectrum = (dot(values, up_ref[...]) + dot(values, low_ref[...])).astype(bf16)
            for q in range(quads):
                spec[q, p * quarter : (p + 1) * quarter, :] = spectrum[:, q * lanes : (q + 1) * lanes]
        pad = pad_tile(rows, opt_pad, lanes)
        for d in range(quads):
            out_refs[d][:opt_main, :] = spec[at_ref[2] ^ d]
            out_refs[d][opt_main:, :] = pad

    opt_out = pl.pallas_call(
        opt_kernel,
        out_shape=[jax.ShapeDtypeStruct((opt_main + opt_pad, lanes), bf16)] * quads,
        in_specs=[smem(), vmem(), vmem(), vmem()],
        out_specs=[vmem()] * quads,
        scratch_shapes=[pltpu.VMEM((quads, opt_main, lanes), bf16)],
        compiler_params=params,
        name="opt_columns",
    )(places, optical, t_upper, t_lower)
    opt_got = exchange(opt_out, ("half", "band"))

    slots = half_count * group_size
    lag_rows = quarter + 2 * peak_count
    columns = patch_dev * band_count * lanes

    sar_count = members if direct else 1

    def middle_kernel(at_ref, dest_ref, peak_ref, stat_ref, up_ref, low_ref, tup_ref, tlow_ref, *rest):
        sar_refs, rest = rest[:sar_count], rest[sar_count:]
        opt_refs, rest = rest[:quads], rest[quads:]
        out_refs, rest = rest[:quads], rest[quads:]
        slot_ref, sar_x, opt_x, sar_stat, opt_stat, sar_y, opt_y, freq, lag, lag_out = rest
        opt_stat[...] = jnp.zeros(opt_stat.shape, f32)
        for d in range(quads):
            source = at_ref[2] ^ d
            b = source % band_count
            start = pl.multiple_of(source // band_count * quarter, quarter)
            for p in range(patch_dev):
                opt_x[p, b, pl.ds(start, quarter), :] = opt_refs[d][p * quarter : (p + 1) * quarter, :]
            opt_stat[b] += opt_refs[d][opt_main:, :].astype(f32)
        base = at_ref[0] * slots
        sar_index = lax.broadcasted_iota(jnp.int32, (sar_pad, lanes), 0)
        opt_index = lax.broadcasted_iota(jnp.int32, (opt_pad, lanes), 0)
        if direct:
            sar_stat[...] = jnp.zeros(sar_stat.shape, f32)

            def place(n, carry):
                offset = dest_ref[n] - base
                inside = (offset >= 0) & (offset < slots)
                at = n // group_size * half_count + offset // group_size
                slot_ref[jnp.where(inside, at, slots)] = offset % group_size
                return carry

            lax.fori_loop(0, group_size * group_size, place, 0)
            for d in range(members):
                source = at_ref[3] ^ d
                b = source % band_count
                stats = sar_refs[d][main_rows:, :].astype(f32)
                for h in range(half_count):
                    slot = slot_ref[source // band_count * half_count + h]
                    p = slot // patch_slots
                    line = h * quarter + slot % patch_slots * block_lines
                    sar_x[p, b, pl.ds(pl.multiple_of(line, block_lines), block_lines), :] = sar_refs[d][
                        h * block_lines : (h + 1) * block_lines, :
                    ]
                    hit = (sar_index >= h * 6) & (sar_index < h * 6 + 6)
                    sar_stat[p, b] += jnp.where(hit, stats, 0.0)
        else:
            for b in range(band_count):
                for p in range(patch_dev):
                    sar_x[p, b] = sar_refs[0][b, p]
        scales = []
        for p in range(patch_dev):
            energies = [jnp.zeros((1, 1), f32), jnp.zeros((1, 1), f32)]
            for b in range(band_count):
                moments = []
                for kind in range(2):
                    first = p * 6 + kind * 3
                    hit = (opt_index >= first) & (opt_index < first + 3)
                    moments.append(jnp.sum(jnp.where(hit, opt_stat[b], 0.0), keepdims=True))
                energies[0] = energies[0] + (moments[1] - moments[0] * moments[0] / pixel_count)
                if direct:
                    moments = []
                    for kind in range(2):
                        hit = (sar_index % 6 // 3 == kind) & (sar_index < 6 * half_count)
                        moments.append(jnp.sum(jnp.where(hit, sar_stat[p, b], 0.0), keepdims=True))
                else:
                    moments = [jnp.full((1, 1), stat_ref[(p * band_count + b) * 2 + kind]) for kind in range(2)]
                energies[1] = energies[1] + (moments[1] - moments[0] * moments[0] / pixel_count)
            energies = [entry / (band_count * pixel_count) for entry in energies]
            scales.append(
                lax.rsqrt(band_count * pixel_count * (energies[0] + EPSILON) * (energies[1] + EPSILON))
                / pixel_count
            )

        def joined(x):
            return jnp.concatenate(
                [x[p, b] for p in range(patch_dev) for b in range(band_count)], axis=1
            )

        opt_y[...] = dot(up_ref[...], joined(opt_x)) + dot(low_ref[...], joined(opt_x))
        sar_y[...] = dot(up_ref[...], joined(sar_x)) + dot(low_ref[...], joined(sar_x))
        lane = lax.broadcasted_iota(jnp.int32, (width, lanes), 1)
        row = lax.broadcasted_iota(jnp.int32, (width, lanes), 0)
        left = lane < width
        real_lane = ((lane == 0) | (lane == width)) & (at_ref[2] == 0)
        weight = jnp.where(real_lane, 2.0, 4.0).astype(f32)
        for p in range(patch_dev):
            for g in range(quads):
                cos_rows = slice(g * lanes, g * lanes + width)
                sin_rows = slice(g * lanes + width, (g + 1) * lanes)
                aa = bb = ab = ra = rb = rab = 0.0
                for b in range(band_count):
                    at = (p * band_count + b) * lanes
                    cut = slice(at, at + lanes)
                    ao, bo = opt_y[cos_rows, cut], opt_y[sin_rows, cut]
                    as_, bs = sar_y[cos_rows, cut], sar_y[sin_rows, cut]
                    ras, rbs = swap_halves(as_), swap_halves(bs)
                    aa = aa + ao * as_
                    bb = bb + bo * bs
                    ab = ab + (ao * bs - bo * as_)
                    ra = ra + ao * ras
                    rb = rb + bo * rbs
                    rab = rab + (ao * rbs - bo * ras)
                even, even_turned = aa + bb, ra + rb
                odd, odd_turned = ab, rab
                scale = weight * scales[p]
                if g == 0:
                    first = row == 0
                    even = jnp.where(first, aa, even)
                    even_turned = jnp.where(first, ra, even_turned)
                    odd = jnp.where(first, bb, odd)
                    odd_turned = jnp.where(first, rb, odd_turned)
                    scale = jnp.where(first, 0.5 * scale, scale)

                def combine(plain, turned):
                    pair = jnp.where(
                        left, plain + swap_halves(plain), swap_halves(turned) - turned
                    )
                    return jnp.where(real_lane, plain, pair) * scale

                even = combine(even, even_turned)
                odd = combine(odd, odd_turned)
                if g == 0:
                    even = jnp.where(first & real_lane & (lane == 0), 0.0, even)
                freq[cos_rows, p * lanes : (p + 1) * lanes] = even
                freq[sin_rows, p * lanes : (p + 1) * lanes] = odd
        upper = freq[...].astype(bf16)
        lower = (freq[...] - upper.astype(f32)).astype(bf16)
        back = dot(tup_ref[...], upper) + dot(tup_ref[...], lower) + dot(tlow_ref[...], upper)
        for p in range(patch_dev):
            lag[p] = back[:, p * lanes : (p + 1) * lanes]
        for b in range(band_count):
            turn = (b - at_ref[1] + band_count) % band_count
            for k in range(kept):
                p = b * kept + k
                picked = jnp.concatenate(
                    [lag[p, pl.ds(peak_ref[turn, k, j], 1), :] for j in range(peak_count)], axis=0
                )
                upper = picked.astype(bf16).astype(f32)
                picked = jnp.concatenate([upper, picked - upper], axis=0).astype(bf16)
                for h in range(half_count):
                    lag_out[h * band_count + b, k, :quarter, :] = lag[
                        p, h * quarter : (h + 1) * quarter, :
                    ].astype(bf16)
                    lag_out[h * band_count + b, k, quarter:, :] = picked
        for d in range(quads):
            out_refs[d][...] = lag_out[at_ref[2] ^ d]

    sar_mid = sar_got if direct else []
    sar_stats = jnp.zeros((2,), f32)
    dest_mid = destination
    if not direct:
        inverse = (
            jnp.zeros_like(destination)
            .at[destination]
            .set(jnp.arange(destination.shape[0], dtype=jnp.int32))
        )
        sources = (
            lax.dynamic_slice_in_dim(inverse, tile_at * slots, slots).reshape(half_count, group_size)
            // group_size
        )
        halves = jnp.arange(half_count, dtype=jnp.int32)[:, None]
        got = sar_got.reshape(group_size, band_count, sar_rows, lanes)
        lines = got[:, :, :main_rows].reshape(
            group_size, band_count, half_count, block_lines, lanes
        )
        lines = jnp.transpose(lines, (0, 2, 1, 3, 4))[sources, halves]
        sar_mid.append(jnp.transpose(
            lines.reshape(half_count, patch_dev, patch_slots, band_count, block_lines, lanes),
            (3, 1, 0, 2, 4, 5),
        ).reshape(band_count, patch_dev, extent, lanes))
        stats = got[:, :, main_rows : main_rows + 6 * half_count].astype(f32)
        stats = stats.reshape(group_size, band_count, half_count, 2, 3 * lanes).sum(axis=-1)
        stats = jnp.transpose(stats, (0, 2, 1, 3))[sources, halves]
        sar_stats = jnp.transpose(
            stats.reshape(half_count, patch_dev, patch_slots, band_count, 2).sum(axis=(0, 2)),
            (0, 1, 2),
        ).reshape(-1)
        dest_mid = destination[:1]

    lag_out = pl.pallas_call(
        middle_kernel,
        out_shape=[jax.ShapeDtypeStruct((kept, lag_rows, lanes), bf16)] * quads,
        in_specs=[smem()] * 4 + [vmem()] * (4 + sar_count + quads),
        out_specs=[vmem()] * quads,
        scratch_shapes=[
            pltpu.SMEM((slots + 1 if direct else 1,), jnp.int32),
            pltpu.VMEM((patch_dev, band_count, extent, lanes), bf16),
            pltpu.VMEM((patch_dev, band_count, extent, lanes), bf16),
            pltpu.VMEM((patch_dev, band_count, sar_pad, lanes), f32),
            pltpu.VMEM((band_count, opt_pad, lanes), f32),
            pltpu.VMEM((extent, columns), f32),
            pltpu.VMEM((extent, columns), f32),
            pltpu.VMEM((extent, patch_dev * lanes), f32),
            pltpu.VMEM((patch_dev, extent, lanes), f32),
            pltpu.VMEM((quads, kept, lag_rows, lanes), bf16),
        ],
        compiler_params=params,
        name="lines_and_cross",
    )(
        places, dest_mid, peak_lines, sar_stats, r_upper, r_lower, t_upper, t_lower, *sar_mid, *opt_got
    )
    lag_got = exchange(lag_out, ("half", "band"))

    def last_kernel(at_ref, peak_ref, up_ref, low_ref, *rest):
        lag_refs, (out_ref, value_ref, lag_ref) = rest[:quads], rest[quads:]
        for d in range(quads):
            lag_ref[at_ref[2] ^ d] = lag_refs[d][...]
        for k in range(kept):
            values = jnp.concatenate([lag_ref[q, k] for q in range(quads)], axis=1)
            result = dot(values, up_ref[...]) + dot(values, low_ref[...])
            out_ref[k] = result[:quarter]
            picked = result[quarter : quarter + peak_count] + result[quarter + peak_count :]
            lane = lax.broadcasted_iota(jnp.int32, (peak_count, extent), 1)
            row = lax.broadcasted_iota(jnp.int32, (peak_count, extent), 0)
            wanted = jnp.zeros((peak_count, extent), jnp.int32)
            for j in range(peak_count):
                wanted = jnp.where(row == j, peak_ref[k, 1, j], wanted)
            chosen = jnp.sum(jnp.where(lane == wanted, picked, 0.0), axis=1, keepdims=True)
            line = jnp.sum(jnp.where(lane == row, chosen, 0.0), axis=0, keepdims=True)
            value_ref[k : k + 1, :] = line[:, :peak_count]

    surface, peak_values = pl.pallas_call(
        last_kernel,
        out_shape=(
            jax.ShapeDtypeStruct((kept, quarter, extent), f32),
            jax.ShapeDtypeStruct((kept, peak_count), f32),
        ),
        in_specs=[smem(), smem()] + [vmem()] * (2 + quads),
        out_specs=(vmem(), vmem()),
        scratch_shapes=[pltpu.VMEM((quads, kept, lag_rows, lanes), bf16)],
        compiler_params=params,
        name="columns_back",
    )(places, peaks, r_upper, r_lower, *lag_got)
    return (surface, peak_values)


def solution(mesh):
    in_specs = (
        P(("scene", "tile"), "band", "half", None),
        P("band", ("scene", "tile", "half"), None),
        P("scene"),
        P(("scene", "tile", "band"), None, None),
    )
    out_specs = (P(("scene", "tile", "band"), "half", None), P(("scene", "tile", "band"), None))
    return jax.shard_map(local, mesh=mesh, in_specs=in_specs, out_specs=out_specs, check_vma=False)
```

```python
import math

import jax
import jax.numpy as jnp
import numpy as np
from jax import lax
from jax.experimental import pallas as pl
from jax.experimental.pallas import tpu as pltpu
from jax.sharding import PartitionSpec as P

EPSILON = 1e-06
f32 = jnp.float32
bf16 = jnp.bfloat16


def packed_table(extent, groups):
    width = extent // 2 // groups
    places = np.arange(extent)
    phases = np.outer(places, np.arange(extent // 2)) % extent
    angles = phases * (2.0 * math.pi / extent)
    cosines = np.cos(angles)
    sines = -np.sin(angles)
    sines[:, 0] = 1.0 - 2.0 * (places % 2)
    table = np.stack(
        [cosines.reshape(extent, groups, width), sines.reshape(extent, groups, width)], axis=2
    ).reshape(extent, extent)
    return table.astype(np.float32)


def table_pair(table):
    upper = table.astype(bf16)
    lower = (table - upper.astype(np.float32)).astype(bf16)
    return (jnp.asarray(upper), jnp.asarray(lower))


def dot(left, right):
    return jnp.dot(left, right, preferred_element_type=f32)


def three_parts(value):
    upper = value.astype(bf16)
    rest = value - upper.astype(f32)
    middle = rest.astype(bf16)
    lower = (rest - middle.astype(f32)).astype(bf16)
    return [upper.astype(f32), middle.astype(f32), lower.astype(f32)]


def stat_rows(values, lanes):
    values = values.astype(f32)
    sums = jnp.sum(values, axis=0, keepdims=True)
    squares = jnp.sum(values * values, axis=0, keepdims=True)
    rows = []
    for row in (sums, squares):
        folded = row[:, :lanes]
        for at in range(lanes, row.shape[1], lanes):
            folded = folded + row[:, at : at + lanes]
        rows += three_parts(folded)
    return rows


def pad_tile(rows, count, lanes):
    index = lax.broadcasted_iota(jnp.int32, (count, lanes), 0)
    tile = jnp.zeros((count, lanes), f32)
    for at, row in enumerate(rows):
        tile = jnp.where(index == at, row, tile)
    return tile.astype(bf16)


def round_up(value, step):
    return (value + step - 1) // step * step


def swap_halves(value):
    width = value.shape[1] // 2
    if value.shape[1] == 128:
        return pltpu.roll(value, width, 1)
    return jnp.concatenate([value[:, width:], value[:, :width]], axis=1)


def exchange(parcels, axes):
    count = len(parcels)
    got = [parcels[0]] + [None] * (count - 1)
    for d in reversed(range(1, count)):
        got[d] = lax.ppermute(parcels[d], axes, [(at, at ^ d) for at in range(count)])
    return got


def vmem():
    return pl.BlockSpec(memory_space=pltpu.VMEM)


def smem():
    return pl.BlockSpec(memory_space=pltpu.SMEM)


def local(optical, sar, destination, peaks):
    tile_count = lax.axis_size("tile")
    half_count = lax.axis_size("half")
    band_count = lax.axis_size("band")
    group_size = tile_count * half_count
    patch_dev, local_bands, quarter, extent = optical.shape
    assert local_bands == 1
    block_lines = sar.shape[1] // group_size
    pixel_count = extent * extent
    kept = patch_dev // band_count
    peak_count = peaks.shape[2]
    quads = half_count * band_count
    lanes = extent // quads
    width = lanes // 2
    patch_slots = quarter // block_lines
    members = tile_count * quads
    direct = block_lines % 16 == 0 and members <= 16
    assert quads & (quads - 1) == 0
    table = packed_table(extent, quads)
    t_upper, t_lower = table_pair(table)
    r_upper, r_lower = table_pair(np.ascontiguousarray(table.T))
    tile_at = lax.axis_index("tile")
    half_at = lax.axis_index("half")
    band_at = lax.axis_index("band")
    device_at = lax.axis_index(("tile", "half"))
    quad_at = half_at * band_count + band_at
    member_at = tile_at * quads + quad_at
    places = jnp.stack([tile_at, band_at, quad_at, member_at])
    params = pltpu.CompilerParams(vmem_limit_bytes=48 * 1024 * 1024)

    peak_list = [peaks]
    for step in range(1, band_count):
        route = [((at + step) % band_count, at) for at in range(band_count)]
        peak_list.append(lax.ppermute(peaks, "band", route))
    peak_lines = jnp.stack([entry[:, 0, :] for entry in peak_list])

    main_rows = half_count * block_lines
    sar_pad = round_up(6 * half_count, 16)
    sar_rows = main_rows + sar_pad

    def sar_kernel(at_ref, dest_ref, sar_hbm, up_hbm, low_hbm, out_ref, token_ref, *rest):
        order_ref, sar_ref, up_ref, low_ref, sems = rest
        copies = [
            pltpu.make_async_copy(source, target, sems.at[n])
            for n, (source, target) in enumerate(
                [(sar_hbm, sar_ref), (up_hbm, up_ref), (low_hbm, low_ref)]
            )
        ]
        for copy in copies:
            copy.start()
        token_ref[...] = jnp.zeros(token_ref.shape, f32)
        if direct:
            for n in range(group_size):
                order_ref[dest_ref[at_ref[0] * group_size + n] // group_size] = n
        copies[0].wait()
        if direct:
            blocks = [
                sar_ref[0, pl.ds(pl.multiple_of(order_ref[g] * block_lines, block_lines), block_lines), :]
                for g in range(group_size)
            ]
            values = jnp.concatenate(blocks, axis=0)
        else:
            values = sar_ref[0]
        for t in range(tile_count):
            rows = []
            for h in range(half_count):
                start = (t * half_count + h) * block_lines
                rows += stat_rows(values[start : start + block_lines], lanes)
            pad = pad_tile(rows, sar_pad, lanes)
            for q in range(quads):
                out_ref[t * quads + q, main_rows:, :] = pad
        copies[1].wait()
        copies[2].wait()
        spectrum = (dot(values, up_ref[...]) + dot(values, low_ref[...])).astype(bf16)
        for t in range(tile_count):
            lines = spectrum[t * main_rows : (t + 1) * main_rows]
            for q in range(quads):
                out_ref[t * quads + q, :main_rows, :] = lines[:, q * lanes : (q + 1) * lanes]

    sar_in = sar
    dest_in = destination
    if not direct:
        own_blocks = lax.dynamic_slice_in_dim(destination, device_at * group_size, group_size)
        order = jnp.argsort(own_blocks // group_size)
        sar_in = jnp.take(
            sar.reshape(group_size, block_lines, extent), order, axis=0
        ).reshape(sar.shape)
        dest_in = own_blocks[:1]
    hbm = pl.BlockSpec(memory_space=pltpu.HBM)
    sar_out, token = pl.pallas_call(
        sar_kernel,
        out_shape=[
            jax.ShapeDtypeStruct((members, sar_rows, lanes), bf16),
            jax.ShapeDtypeStruct((8, 128), f32),
        ],
        in_specs=[smem(), smem(), hbm, hbm, hbm],
        out_specs=[vmem(), vmem()],
        scratch_shapes=[
            pltpu.SMEM((group_size,), jnp.int32),
            pltpu.VMEM(sar.shape, bf16),
            pltpu.VMEM((extent, extent), bf16),
            pltpu.VMEM((extent, extent), bf16),
            pltpu.SemaphoreType.DMA((3,)),
        ],
        compiler_params=params,
        name="sar_columns",
    )(device_at.reshape(1), dest_in, sar_in, t_upper, t_lower)
    sar_got = lax.all_to_all(
        sar_out, ("tile", "half", "band"), split_axis=0, concat_axis=0, tiled=True
    )

    opt_main = patch_dev * quarter
    opt_pad = round_up(6 * patch_dev, 16)

    def opt_kernel(at_ref, token_ref, opt_ref, up_ref, low_ref, *rest):
        out_refs, spec = rest[:-1], rest[-1]
        rows = []
        for p in range(patch_dev):
            values = opt_ref[p, 0]
            rows += stat_rows(values, lanes)
            spectrum = (dot(values, up_ref[...]) + dot(values, low_ref[...])).astype(bf16)
            for q in range(quads):
                spec[q, p * quarter : (p + 1) * quarter, :] = spectrum[:, q * lanes : (q + 1) * lanes]
        pad = pad_tile(rows, opt_pad, lanes)
        for d in range(quads):
            out_refs[d][:opt_main, :] = spec[at_ref[2] ^ d]
            out_refs[d][opt_main:, :] = pad

    opt_out = pl.pallas_call(
        opt_kernel,
        out_shape=[jax.ShapeDtypeStruct((opt_main + opt_pad, lanes), bf16)] * quads,
        in_specs=[smem(), vmem(), vmem(), vmem(), vmem()],
        out_specs=[vmem()] * quads,
        scratch_shapes=[pltpu.VMEM((quads, opt_main, lanes), bf16)],
        compiler_params=params,
        name="opt_columns",
    )(places, token, optical, t_upper, t_lower)
    opt_got = exchange(opt_out, ("half", "band"))

    slots = half_count * group_size
    lag_rows = quarter + 2 * peak_count
    columns = patch_dev * band_count * lanes

    def joined(x):
        return jnp.concatenate([x[p, b] for p in range(patch_dev) for b in range(band_count)], axis=1)

    def opt_lines_kernel(at_ref, up_ref, low_ref, *rest):
        opt_refs, (opt_y, opt_stat, opt_x) = rest[:quads], rest[quads:]
        opt_stat[...] = jnp.zeros(opt_stat.shape, f32)
        for d in range(quads):
            source = at_ref[2] ^ d
            b = source % band_count
            start = pl.multiple_of(source // band_count * quarter, quarter)
            for p in range(patch_dev):
                opt_x[p, b, pl.ds(start, quarter), :] = opt_refs[d][p * quarter : (p + 1) * quarter, :]
            opt_stat[b] += opt_refs[d][opt_main:, :].astype(f32)
        values = joined(opt_x)
        opt_y[...] = dot(up_ref[...], values) + dot(low_ref[...], values)

    opt_y, opt_stat = pl.pallas_call(
        opt_lines_kernel,
        out_shape=[
            jax.ShapeDtypeStruct((extent, columns), f32),
            jax.ShapeDtypeStruct((band_count, opt_pad, lanes), f32),
        ],
        in_specs=[smem()] + [vmem()] * (2 + quads),
        out_specs=[vmem(), vmem()],
        scratch_shapes=[pltpu.VMEM((patch_dev, band_count, extent, lanes), bf16)],
        compiler_params=params,
        name="opt_lines",
    )(places, r_upper, r_lower, *opt_got)

    def middle_kernel(
        at_ref, dest_ref, peak_ref, stat_ref, up_ref, low_ref, tup_ref, tlow_ref,
        sar_ref, opt_y, opt_stat, *rest,
    ):
        out_refs, rest = rest[:quads], rest[quads:]
        slot_ref, sar_x, sar_stat, sar_y, freq, lag, lag_out = rest
        base = at_ref[0] * slots
        sar_index = lax.broadcasted_iota(jnp.int32, (sar_pad, lanes), 0)
        opt_index = lax.broadcasted_iota(jnp.int32, (opt_pad, lanes), 0)
        if direct:
            sar_stat[...] = jnp.zeros(sar_stat.shape, f32)

            def place(n, carry):
                offset = dest_ref[n] - base
                inside = (offset >= 0) & (offset < slots)
                at = n // group_size * half_count + offset // group_size
                slot_ref[jnp.where(inside, at, slots)] = offset % group_size
                return carry

            lax.fori_loop(0, group_size * group_size, place, 0)
            for source in range(members):
                b = source % band_count
                stats = sar_ref[source, main_rows:, :].astype(f32)
                for h in range(half_count):
                    slot = slot_ref[source // band_count * half_count + h]
                    p = slot // patch_slots
                    line = h * quarter + slot % patch_slots * block_lines
                    sar_x[p, b, pl.ds(pl.multiple_of(line, block_lines), block_lines), :] = sar_ref[
                        source, h * block_lines : (h + 1) * block_lines, :
                    ]
                    hit = (sar_index >= h * 6) & (sar_index < h * 6 + 6)
                    sar_stat[p, b] += jnp.where(hit, stats, 0.0)
        else:
            for b in range(band_count):
                for p in range(patch_dev):
                    sar_x[p, b] = sar_ref[b, p]
        scales = []
        for p in range(patch_dev):
            energies = [jnp.zeros((1, 1), f32), jnp.zeros((1, 1), f32)]
            for b in range(band_count):
                moments = []
                for kind in range(2):
                    first = p * 6 + kind * 3
                    hit = (opt_index >= first) & (opt_index < first + 3)
                    moments.append(jnp.sum(jnp.where(hit, opt_stat[b], 0.0), keepdims=True))
                energies[0] = energies[0] + (moments[1] - moments[0] * moments[0] / pixel_count)
                if direct:
                    moments = []
                    for kind in range(2):
                        hit = (sar_index % 6 // 3 == kind) & (sar_index < 6 * half_count)
                        moments.append(jnp.sum(jnp.where(hit, sar_stat[p, b], 0.0), keepdims=True))
                else:
                    moments = [jnp.full((1, 1), stat_ref[(p * band_count + b) * 2 + kind]) for kind in range(2)]
                energies[1] = energies[1] + (moments[1] - moments[0] * moments[0] / pixel_count)
            energies = [entry / (band_count * pixel_count) for entry in energies]
            scales.append(
                lax.rsqrt(band_count * pixel_count * (energies[0] + EPSILON) * (energies[1] + EPSILON))
                / pixel_count
            )

        sar_y[...] = dot(up_ref[...], joined(sar_x)) + dot(low_ref[...], joined(sar_x))
        lane = lax.broadcasted_iota(jnp.int32, (width, lanes), 1)
        row = lax.broadcasted_iota(jnp.int32, (width, lanes), 0)
        left = lane < width
        real_lane = ((lane == 0) | (lane == width)) & (at_ref[2] == 0)
        weight = jnp.where(real_lane, 2.0, 4.0).astype(f32)
        for p in range(patch_dev):
            for g in range(quads):
                cos_rows = slice(g * lanes, g * lanes + width)
                sin_rows = slice(g * lanes + width, (g + 1) * lanes)
                aa = bb = ab = ra = rb = rab = 0.0
                for b in range(band_count):
                    at = (p * band_count + b) * lanes
                    cut = slice(at, at + lanes)
                    ao, bo = opt_y[cos_rows, cut], opt_y[sin_rows, cut]
                    as_, bs = sar_y[cos_rows, cut], sar_y[sin_rows, cut]
                    ras, rbs = swap_halves(as_), swap_halves(bs)
                    aa = aa + ao * as_
                    bb = bb + bo * bs
                    ab = ab + (ao * bs - bo * as_)
                    ra = ra + ao * ras
                    rb = rb + bo * rbs
                    rab = rab + (ao * rbs - bo * ras)
                even, even_turned = aa + bb, ra + rb
                odd, odd_turned = ab, rab
                scale = weight * scales[p]
                if g == 0:
                    first = row == 0
                    even = jnp.where(first, aa, even)
                    even_turned = jnp.where(first, ra, even_turned)
                    odd = jnp.where(first, bb, odd)
                    odd_turned = jnp.where(first, rb, odd_turned)
                    scale = jnp.where(first, 0.5 * scale, scale)

                def combine(plain, turned):
                    pair = jnp.where(
                        left, plain + swap_halves(plain), swap_halves(turned) - turned
                    )
                    return jnp.where(real_lane, plain, pair) * scale

                even = combine(even, even_turned)
                odd = combine(odd, odd_turned)
                if g == 0:
                    even = jnp.where(first & real_lane & (lane == 0), 0.0, even)
                freq[cos_rows, p * lanes : (p + 1) * lanes] = even
                freq[sin_rows, p * lanes : (p + 1) * lanes] = odd
        upper = freq[...].astype(bf16)
        lower = (freq[...] - upper.astype(f32)).astype(bf16)
        back = dot(tup_ref[...], upper) + dot(tup_ref[...], lower) + dot(tlow_ref[...], upper)
        for p in range(patch_dev):
            lag[p] = back[:, p * lanes : (p + 1) * lanes]
        for b in range(band_count):
            turn = (b - at_ref[1] + band_count) % band_count
            for k in range(kept):
                p = b * kept + k
                picked = jnp.concatenate(
                    [lag[p, pl.ds(peak_ref[turn, k, j], 1), :] for j in range(peak_count)], axis=0
                )
                upper = picked.astype(bf16).astype(f32)
                picked = jnp.concatenate([upper, picked - upper], axis=0).astype(bf16)
                for h in range(half_count):
                    lag_out[h * band_count + b, k, :quarter, :] = lag[
                        p, h * quarter : (h + 1) * quarter, :
                    ].astype(bf16)
                    lag_out[h * band_count + b, k, quarter:, :] = picked
        for d in range(quads):
            out_refs[d][...] = lag_out[at_ref[2] ^ d]

    sar_mid = sar_got
    sar_stats = jnp.zeros((2,), f32)
    dest_mid = destination
    if not direct:
        inverse = (
            jnp.zeros_like(destination)
            .at[destination]
            .set(jnp.arange(destination.shape[0], dtype=jnp.int32))
        )
        sources = (
            lax.dynamic_slice_in_dim(inverse, tile_at * slots, slots).reshape(half_count, group_size)
            // group_size
        )
        halves = jnp.arange(half_count, dtype=jnp.int32)[:, None]
        got = sar_got.reshape(group_size, band_count, sar_rows, lanes)
        lines = got[:, :, :main_rows].reshape(
            group_size, band_count, half_count, block_lines, lanes
        )
        lines = jnp.transpose(lines, (0, 2, 1, 3, 4))[sources, halves]
        sar_mid = jnp.transpose(
            lines.reshape(half_count, patch_dev, patch_slots, band_count, block_lines, lanes),
            (3, 1, 0, 2, 4, 5),
        ).reshape(band_count, patch_dev, extent, lanes)
        stats = got[:, :, main_rows : main_rows + 6 * half_count].astype(f32)
        stats = stats.reshape(group_size, band_count, half_count, 2, 3 * lanes).sum(axis=-1)
        stats = jnp.transpose(stats, (0, 2, 1, 3))[sources, halves]
        sar_stats = jnp.transpose(
            stats.reshape(half_count, patch_dev, patch_slots, band_count, 2).sum(axis=(0, 2)),
            (0, 1, 2),
        ).reshape(-1)
        dest_mid = destination[:1]

    lag_out = pl.pallas_call(
        middle_kernel,
        out_shape=[jax.ShapeDtypeStruct((kept, lag_rows, lanes), bf16)] * quads,
        in_specs=[smem()] * 4 + [vmem()] * 7,
        out_specs=[vmem()] * quads,
        scratch_shapes=[
            pltpu.SMEM((slots + 1 if direct else 1,), jnp.int32),
            pltpu.VMEM((patch_dev, band_count, extent, lanes), bf16),
            pltpu.VMEM((patch_dev, band_count, sar_pad, lanes), f32),
            pltpu.VMEM((extent, columns), f32),
            pltpu.VMEM((extent, patch_dev * lanes), f32),
            pltpu.VMEM((patch_dev, extent, lanes), f32),
            pltpu.VMEM((quads, kept, lag_rows, lanes), bf16),
        ],
        compiler_params=params,
        name="lines_and_cross",
    )(
        places, dest_mid, peak_lines, sar_stats, r_upper, r_lower, t_upper, t_lower,
        sar_mid, opt_y, opt_stat,
    )
    lag_got = exchange(lag_out, ("half", "band"))

    def last_kernel(at_ref, peak_ref, up_ref, low_ref, *rest):
        lag_refs, (out_ref, value_ref, lag_ref) = rest[:quads], rest[quads:]
        for d in range(quads):
            lag_ref[at_ref[2] ^ d] = lag_refs[d][...]
        for k in range(kept):
            values = jnp.concatenate([lag_ref[q, k] for q in range(quads)], axis=1)
            result = dot(values, up_ref[...]) + dot(values, low_ref[...])
            out_ref[k] = result[:quarter]
            picked = result[quarter : quarter + peak_count] + result[quarter + peak_count :]
            lane = lax.broadcasted_iota(jnp.int32, (peak_count, extent), 1)
            row = lax.broadcasted_iota(jnp.int32, (peak_count, extent), 0)
            wanted = jnp.zeros((peak_count, extent), jnp.int32)
            for j in range(peak_count):
                wanted = jnp.where(row == j, peak_ref[k, 1, j], wanted)
            chosen = jnp.sum(jnp.where(lane == wanted, picked, 0.0), axis=1, keepdims=True)
            line = jnp.sum(jnp.where(lane == row, chosen, 0.0), axis=0, keepdims=True)
            value_ref[k : k + 1, :] = line[:, :peak_count]

    surface, peak_values = pl.pallas_call(
        last_kernel,
        out_shape=(
            jax.ShapeDtypeStruct((kept, quarter, extent), f32),
            jax.ShapeDtypeStruct((kept, peak_count), f32),
        ),
        in_specs=[smem(), smem()] + [vmem()] * (2 + quads),
        out_specs=(vmem(), vmem()),
        scratch_shapes=[pltpu.VMEM((quads, kept, lag_rows, lanes), bf16)],
        compiler_params=params,
        name="columns_back",
    )(places, peaks, r_upper, r_lower, *lag_got)
    return (surface, peak_values)


def solution(mesh):
    in_specs = (
        P(("scene", "tile"), "band", "half", None),
        P("band", ("scene", "tile", "half"), None),
        P("scene"),
        P(("scene", "tile", "band"), None, None),
    )
    out_specs = (P(("scene", "tile", "band"), "half", None), P(("scene", "tile", "band"), None))
    return jax.shard_map(local, mesh=mesh, in_specs=in_specs, out_specs=out_specs, check_vma=False)
```

```python
import math

import jax
import jax.numpy as jnp
import numpy as np
from jax import lax
from jax.experimental import pallas as pl
from jax.experimental.pallas import tpu as pltpu
from jax.sharding import PartitionSpec as P

EPSILON = 1e-06
f32 = jnp.float32
bf16 = jnp.bfloat16


def packed_table(extent, groups):
    width = extent // 2 // groups
    places = np.arange(extent)
    phases = np.outer(places, np.arange(extent // 2)) % extent
    angles = phases * (2.0 * math.pi / extent)
    cosines = np.cos(angles)
    sines = -np.sin(angles)
    sines[:, 0] = 1.0 - 2.0 * (places % 2)
    table = np.stack(
        [cosines.reshape(extent, groups, width), sines.reshape(extent, groups, width)], axis=2
    ).reshape(extent, extent)
    return table.astype(np.float32)


def table_pair(table):
    upper = table.astype(bf16)
    lower = (table - upper.astype(np.float32)).astype(bf16)
    return (jnp.asarray(upper), jnp.asarray(lower))


def dot(left, right):
    return jnp.dot(left, right, preferred_element_type=f32)


def three_parts(value):
    upper = value.astype(bf16)
    rest = value - upper.astype(f32)
    middle = rest.astype(bf16)
    lower = (rest - middle.astype(f32)).astype(bf16)
    return [upper.astype(f32), middle.astype(f32), lower.astype(f32)]


def stat_rows(values, lanes):
    values = values.astype(f32)
    sums = jnp.sum(values, axis=0, keepdims=True)
    squares = jnp.sum(values * values, axis=0, keepdims=True)
    rows = []
    for row in (sums, squares):
        folded = row[:, :lanes]
        for at in range(lanes, row.shape[1], lanes):
            folded = folded + row[:, at : at + lanes]
        rows += three_parts(folded)
    return rows


def pad_tile(rows, count, lanes):
    index = lax.broadcasted_iota(jnp.int32, (count, lanes), 0)
    tile = jnp.zeros((count, lanes), f32)
    for at, row in enumerate(rows):
        tile = jnp.where(index == at, row, tile)
    return tile.astype(bf16)


def round_up(value, step):
    return (value + step - 1) // step * step


def swap_halves(value):
    width = value.shape[1] // 2
    if value.shape[1] == 128:
        return pltpu.roll(value, width, 1)
    return jnp.concatenate([value[:, width:], value[:, :width]], axis=1)


def exchange(parcels, axes):
    count = len(parcels)
    got = [parcels[0]] + [None] * (count - 1)
    for d in reversed(range(1, count)):
        got[d] = lax.ppermute(parcels[d], axes, [(at, at ^ d) for at in range(count)])
    return got


def vmem():
    return pl.BlockSpec(memory_space=pltpu.VMEM)


def smem():
    return pl.BlockSpec(memory_space=pltpu.SMEM)


def local(optical, sar, destination, peaks):
    tile_count = lax.axis_size("tile")
    half_count = lax.axis_size("half")
    band_count = lax.axis_size("band")
    group_size = tile_count * half_count
    patch_dev, local_bands, quarter, extent = optical.shape
    assert local_bands == 1
    block_lines = sar.shape[1] // group_size
    pixel_count = extent * extent
    kept = patch_dev // band_count
    peak_count = peaks.shape[2]
    quads = half_count * band_count
    lanes = extent // quads
    width = lanes // 2
    patch_slots = quarter // block_lines
    members = tile_count * quads
    direct = block_lines % 16 == 0 and members <= 16
    assert quads & (quads - 1) == 0
    table = packed_table(extent, quads)
    t_upper, t_lower = table_pair(table)
    r_upper, r_lower = table_pair(np.ascontiguousarray(table.T))
    tile_at = lax.axis_index("tile")
    half_at = lax.axis_index("half")
    band_at = lax.axis_index("band")
    device_at = lax.axis_index(("tile", "half"))
    quad_at = half_at * band_count + band_at
    member_at = tile_at * quads + quad_at
    places = jnp.stack([tile_at, band_at, quad_at, member_at])
    params = pltpu.CompilerParams(vmem_limit_bytes=48 * 1024 * 1024)

    peak_list = [peaks]
    for step in range(1, band_count):
        route = [((at + step) % band_count, at) for at in range(band_count)]
        peak_list.append(lax.ppermute(peaks, "band", route))
    peak_lines = jnp.stack([entry[:, 0, :] for entry in peak_list])

    main_rows = half_count * block_lines
    sar_pad = 8
    fold = lanes // half_count
    sar_rows = main_rows + sar_pad

    def sar_kernel(at_ref, dest_ref, sar_hbm, up_hbm, low_hbm, out_ref, token_ref, *rest):
        order_ref, sar_ref, up_ref, low_ref, sems = rest
        copies = [
            pltpu.make_async_copy(source, target, sems.at[n])
            for n, (source, target) in enumerate(
                [(sar_hbm, sar_ref), (up_hbm, up_ref), (low_hbm, low_ref)]
            )
        ]
        for copy in copies:
            copy.start()
        token_ref[...] = jnp.zeros(token_ref.shape, f32)
        if direct:
            for n in range(group_size):
                order_ref[dest_ref[at_ref[0] * group_size + n] // group_size] = n
        copies[0].wait()
        if direct:
            blocks = [
                sar_ref[0, pl.ds(pl.multiple_of(order_ref[g] * block_lines, block_lines), block_lines), :]
                for g in range(group_size)
            ]
            values = jnp.concatenate(blocks, axis=0)
        else:
            values = sar_ref[0]
        for t in range(tile_count):
            rows = []
            for h in range(half_count):
                start = (t * half_count + h) * block_lines
                rows.append(stat_rows(values[start : start + block_lines], fold))
            rows = [jnp.concatenate(parts, axis=1) for parts in zip(*rows)]
            pad = pad_tile(rows, sar_pad, lanes)
            for q in range(quads):
                out_ref[t * quads + q, main_rows:, :] = pad
        copies[1].wait()
        copies[2].wait()
        spectrum = (dot(values, up_ref[...]) + dot(values, low_ref[...])).astype(bf16)
        for t in range(tile_count):
            lines = spectrum[t * main_rows : (t + 1) * main_rows]
            for q in range(quads):
                out_ref[t * quads + q, :main_rows, :] = lines[:, q * lanes : (q + 1) * lanes]

    sar_in = sar
    dest_in = destination
    if not direct:
        own_blocks = lax.dynamic_slice_in_dim(destination, device_at * group_size, group_size)
        order = jnp.argsort(own_blocks // group_size)
        sar_in = jnp.take(
            sar.reshape(group_size, block_lines, extent), order, axis=0
        ).reshape(sar.shape)
        dest_in = own_blocks[:1]
    hbm = pl.BlockSpec(memory_space=pltpu.HBM)
    sar_out, token = pl.pallas_call(
        sar_kernel,
        out_shape=[
            jax.ShapeDtypeStruct((members, sar_rows, lanes), bf16),
            jax.ShapeDtypeStruct((8, 128), f32),
        ],
        in_specs=[smem(), smem(), hbm, hbm, hbm],
        out_specs=[vmem(), vmem()],
        scratch_shapes=[
            pltpu.SMEM((group_size,), jnp.int32),
            pltpu.VMEM(sar.shape, bf16),
            pltpu.VMEM((extent, extent), bf16),
            pltpu.VMEM((extent, extent), bf16),
            pltpu.SemaphoreType.DMA((3,)),
        ],
        compiler_params=params,
        name="sar_columns",
    )(
        device_at.reshape(1),
        dest_in,
        *[pltpu.with_memory_space_constraint(x, pltpu.HBM) for x in (sar_in, t_upper, t_lower)],
    )
    sar_got = lax.all_to_all(
        sar_out, ("tile", "half", "band"), split_axis=0, concat_axis=0, tiled=True
    )

    opt_main = patch_dev * quarter
    opt_pad = round_up(6 * patch_dev, 16)

    def opt_kernel(at_ref, token_ref, opt_ref, up_ref, low_ref, *rest):
        out_refs, spec = rest[:-1], rest[-1]
        rows = []
        for p in range(patch_dev):
            values = opt_ref[p, 0]
            rows += stat_rows(values, lanes)
            spectrum = (dot(values, up_ref[...]) + dot(values, low_ref[...])).astype(bf16)
            for q in range(quads):
                spec[q, p * quarter : (p + 1) * quarter, :] = spectrum[:, q * lanes : (q + 1) * lanes]
        pad = pad_tile(rows, opt_pad, lanes)
        for d in range(quads):
            out_refs[d][:opt_main, :] = spec[at_ref[2] ^ d]
            out_refs[d][opt_main:, :] = pad

    opt_out = pl.pallas_call(
        opt_kernel,
        out_shape=[jax.ShapeDtypeStruct((opt_main + opt_pad, lanes), bf16)] * quads,
        in_specs=[smem(), vmem(), vmem(), vmem(), vmem()],
        out_specs=[vmem()] * quads,
        scratch_shapes=[pltpu.VMEM((quads, opt_main, lanes), bf16)],
        compiler_params=params,
        name="opt_columns",
    )(places, token, optical, t_upper, t_lower)
    opt_got = exchange(opt_out, ("half", "band"))

    slots = half_count * group_size
    lag_rows = quarter + 2 * peak_count
    columns = patch_dev * band_count * lanes

    def joined(x):
        return jnp.concatenate([x[p, b] for p in range(patch_dev) for b in range(band_count)], axis=1)

    def opt_lines(at_ref, up_ref, low_ref, *rest):
        opt_refs, (opt_y, opt_stat, opt_x) = rest[:quads], rest[quads:]
        opt_stat[...] = jnp.zeros(opt_stat.shape, f32)
        for d in range(quads):
            source = at_ref[2] ^ d
            b = source % band_count
            start = pl.multiple_of(source // band_count * quarter, quarter)
            for p in range(patch_dev):
                opt_x[p, b, pl.ds(start, quarter), :] = opt_refs[d][p * quarter : (p + 1) * quarter, :]
            opt_stat[b] += opt_refs[d][opt_main:, :].astype(f32)
        values = joined(opt_x)
        opt_y[...] = dot(up_ref[...], values) + dot(low_ref[...], values)

    def middle_kernel(
        at_ref, dest_ref, peak_ref, stat_ref, up_ref, low_ref, tup_ref, tlow_ref,
        sar_ref, *rest,
    ):
        opt_refs, rest = rest[:quads], rest[quads:]
        out_refs, rest = rest[:quads], rest[quads:]
        slot_ref, sar_x, sar_stat, sar_y, freq, lag, lag_out, opt_y, opt_stat, opt_x = rest
        opt_lines(at_ref, up_ref, low_ref, *opt_refs, opt_y, opt_stat, opt_x)
        base = at_ref[0] * slots
        sar_index = lax.broadcasted_iota(jnp.int32, (sar_pad, lanes), 0)
        sar_lane = lax.broadcasted_iota(jnp.int32, (sar_pad, lanes), 1)
        opt_index = lax.broadcasted_iota(jnp.int32, (opt_pad, lanes), 0)
        if direct:
            sar_stat[...] = jnp.zeros(sar_stat.shape, f32)

            def place(n, carry):
                offset = dest_ref[n] - base
                inside = (offset >= 0) & (offset < slots)
                at = n // group_size * half_count + offset // group_size
                slot_ref[jnp.where(inside, at, slots)] = offset % group_size
                return carry

            lax.fori_loop(0, group_size * group_size, place, 0)
            for source in range(members):
                b = source % band_count
                stats = sar_ref[source, main_rows:, :].astype(f32)
                for h in range(half_count):
                    slot = slot_ref[source // band_count * half_count + h]
                    p = slot // patch_slots
                    line = h * quarter + slot % patch_slots * block_lines
                    sar_x[p, b, pl.ds(pl.multiple_of(line, block_lines), block_lines), :] = sar_ref[
                        source, h * block_lines : (h + 1) * block_lines, :
                    ]
                    hit = (sar_lane >= h * fold) & (sar_lane < (h + 1) * fold)
                    sar_stat[p, b] += jnp.where(hit, stats, 0.0)
        else:
            for b in range(band_count):
                for p in range(patch_dev):
                    sar_x[p, b] = sar_ref[b, p]
        scales = []
        for p in range(patch_dev):
            energies = [jnp.zeros((1, 1), f32), jnp.zeros((1, 1), f32)]
            for b in range(band_count):
                moments = []
                for kind in range(2):
                    first = p * 6 + kind * 3
                    hit = (opt_index >= first) & (opt_index < first + 3)
                    moments.append(jnp.sum(jnp.where(hit, opt_stat[b], 0.0), keepdims=True))
                energies[0] = energies[0] + (moments[1] - moments[0] * moments[0] / pixel_count)
                if direct:
                    moments = []
                    for kind in range(2):
                        hit = (sar_index >= 3 * kind) & (sar_index < 3 * kind + 3)
                        moments.append(jnp.sum(jnp.where(hit, sar_stat[p, b], 0.0), keepdims=True))
                else:
                    moments = [jnp.full((1, 1), stat_ref[(p * band_count + b) * 2 + kind]) for kind in range(2)]
                energies[1] = energies[1] + (moments[1] - moments[0] * moments[0] / pixel_count)
            energies = [entry / (band_count * pixel_count) for entry in energies]
            scales.append(
                lax.rsqrt(band_count * pixel_count * (energies[0] + EPSILON) * (energies[1] + EPSILON))
                / pixel_count
            )

        sar_y[...] = dot(up_ref[...], joined(sar_x)) + dot(low_ref[...], joined(sar_x))
        lane = lax.broadcasted_iota(jnp.int32, (width, lanes), 1)
        row = lax.broadcasted_iota(jnp.int32, (width, lanes), 0)
        left = lane < width
        real_lane = ((lane == 0) | (lane == width)) & (at_ref[2] == 0)
        weight = jnp.where(real_lane, 2.0, 4.0).astype(f32)
        for p in range(patch_dev):
            for g in range(quads):
                cos_rows = slice(g * lanes, g * lanes + width)
                sin_rows = slice(g * lanes + width, (g + 1) * lanes)
                aa = bb = ab = ra = rb = rab = 0.0
                for b in range(band_count):
                    at = (p * band_count + b) * lanes
                    cut = slice(at, at + lanes)
                    ao, bo = opt_y[cos_rows, cut], opt_y[sin_rows, cut]
                    as_, bs = sar_y[cos_rows, cut], sar_y[sin_rows, cut]
                    ras, rbs = swap_halves(as_), swap_halves(bs)
                    aa = aa + ao * as_
                    bb = bb + bo * bs
                    ab = ab + (ao * bs - bo * as_)
                    ra = ra + ao * ras
                    rb = rb + bo * rbs
                    rab = rab + (ao * rbs - bo * ras)
                even, even_turned = aa + bb, ra + rb
                odd, odd_turned = ab, rab
                scale = weight * scales[p]
                if g == 0:
                    first = row == 0
                    even = jnp.where(first, aa, even)
                    even_turned = jnp.where(first, ra, even_turned)
                    odd = jnp.where(first, bb, odd)
                    odd_turned = jnp.where(first, rb, odd_turned)
                    scale = jnp.where(first, 0.5 * scale, scale)

                def combine(plain, turned):
                    pair = jnp.where(
                        left, plain + swap_halves(plain), swap_halves(turned) - turned
                    )
                    return jnp.where(real_lane, plain, pair) * scale

                even = combine(even, even_turned)
                odd = combine(odd, odd_turned)
                if g == 0:
                    even = jnp.where(first & real_lane & (lane == 0), 0.0, even)
                freq[cos_rows, p * lanes : (p + 1) * lanes] = even
                freq[sin_rows, p * lanes : (p + 1) * lanes] = odd
        upper = freq[...].astype(bf16)
        lower = (freq[...] - upper.astype(f32)).astype(bf16)
        back = dot(tup_ref[...], upper) + dot(tup_ref[...], lower) + dot(tlow_ref[...], upper)
        for p in range(patch_dev):
            lag[p] = back[:, p * lanes : (p + 1) * lanes]
        for b in range(band_count):
            turn = (b - at_ref[1] + band_count) % band_count
            for k in range(kept):
                p = b * kept + k
                picked = jnp.concatenate(
                    [lag[p, pl.ds(peak_ref[turn, k, j], 1), :] for j in range(peak_count)], axis=0
                )
                upper = picked.astype(bf16).astype(f32)
                picked = jnp.concatenate([upper, picked - upper], axis=0).astype(bf16)
                for h in range(half_count):
                    lag_out[h * band_count + b, k, :quarter, :] = lag[
                        p, h * quarter : (h + 1) * quarter, :
                    ].astype(bf16)
                    lag_out[h * band_count + b, k, quarter:, :] = picked
        for d in range(quads):
            out_refs[d][...] = lag_out[at_ref[2] ^ d]

    sar_mid = sar_got
    sar_stats = jnp.zeros((2,), f32)
    dest_mid = destination
    if not direct:
        inverse = (
            jnp.zeros_like(destination)
            .at[destination]
            .set(jnp.arange(destination.shape[0], dtype=jnp.int32))
        )
        sources = (
            lax.dynamic_slice_in_dim(inverse, tile_at * slots, slots).reshape(half_count, group_size)
            // group_size
        )
        halves = jnp.arange(half_count, dtype=jnp.int32)[:, None]
        got = sar_got.reshape(group_size, band_count, sar_rows, lanes)
        lines = got[:, :, :main_rows].reshape(
            group_size, band_count, half_count, block_lines, lanes
        )
        lines = jnp.transpose(lines, (0, 2, 1, 3, 4))[sources, halves]
        sar_mid = jnp.transpose(
            lines.reshape(half_count, patch_dev, patch_slots, band_count, block_lines, lanes),
            (3, 1, 0, 2, 4, 5),
        ).reshape(band_count, patch_dev, extent, lanes)
        stats = got[:, :, main_rows : main_rows + 6].astype(f32)
        stats = stats.reshape(group_size, band_count, 2, 3, half_count, fold).sum(axis=(3, 5))
        stats = jnp.transpose(stats, (0, 3, 1, 2))[sources, halves]
        sar_stats = jnp.transpose(
            stats.reshape(half_count, patch_dev, patch_slots, band_count, 2).sum(axis=(0, 2)),
            (0, 1, 2),
        ).reshape(-1)
        dest_mid = destination[:1]

    lag_out = pl.pallas_call(
        middle_kernel,
        out_shape=[jax.ShapeDtypeStruct((kept, lag_rows, lanes), bf16)] * quads,
        in_specs=[smem()] * 4 + [vmem()] * (5 + quads),
        out_specs=[vmem()] * quads,
        scratch_shapes=[
            pltpu.SMEM((slots + 1 if direct else 1,), jnp.int32),
            pltpu.VMEM((patch_dev, band_count, extent, lanes), bf16),
            pltpu.VMEM((patch_dev, band_count, sar_pad, lanes), f32),
            pltpu.VMEM((extent, columns), f32),
            pltpu.VMEM((extent, patch_dev * lanes), f32),
            pltpu.VMEM((patch_dev, extent, lanes), f32),
            pltpu.VMEM((quads, kept, lag_rows, lanes), bf16),
            pltpu.VMEM((extent, columns), f32),
            pltpu.VMEM((band_count, opt_pad, lanes), f32),
            pltpu.VMEM((patch_dev, band_count, extent, lanes), bf16),
        ],
        compiler_params=params,
        name="lines_and_cross",
    )(
        places, dest_mid, peak_lines, sar_stats, r_upper, r_lower, t_upper, t_lower,
        sar_mid, *opt_got,
    )
    lag_got = exchange(lag_out, ("half", "band"))

    def last_kernel(at_ref, peak_ref, up_ref, low_ref, *rest):
        lag_refs, (out_ref, value_ref, lag_ref) = rest[:quads], rest[quads:]
        for d in range(quads):
            lag_ref[at_ref[2] ^ d] = lag_refs[d][...]
        for k in range(kept):
            values = jnp.concatenate([lag_ref[q, k] for q in range(quads)], axis=1)
            result = dot(values, up_ref[...]) + dot(values, low_ref[...])
            out_ref[k] = result[:quarter]
            picked = result[quarter : quarter + peak_count] + result[quarter + peak_count :]
            lane = lax.broadcasted_iota(jnp.int32, (peak_count, extent), 1)
            row = lax.broadcasted_iota(jnp.int32, (peak_count, extent), 0)
            wanted = jnp.zeros((peak_count, extent), jnp.int32)
            for j in range(peak_count):
                wanted = jnp.where(row == j, peak_ref[k, 1, j], wanted)
            chosen = jnp.sum(jnp.where(lane == wanted, picked, 0.0), axis=1, keepdims=True)
            line = jnp.sum(jnp.where(lane == row, chosen, 0.0), axis=0, keepdims=True)
            value_ref[k : k + 1, :] = line[:, :peak_count]

    surface, peak_values = pl.pallas_call(
        last_kernel,
        out_shape=(
            jax.ShapeDtypeStruct((kept, quarter, extent), f32),
            jax.ShapeDtypeStruct((kept, peak_count), f32),
        ),
        in_specs=[smem(), smem()] + [vmem()] * (2 + quads),
        out_specs=(vmem(), vmem()),
        scratch_shapes=[pltpu.VMEM((quads, kept, lag_rows, lanes), bf16)],
        compiler_params=params,
        name="columns_back",
    )(places, peaks, r_upper, r_lower, *lag_got)
    return (surface, peak_values)


def solution(mesh):
    in_specs = (
        P(("scene", "tile"), "band", "half", None),
        P("band", ("scene", "tile", "half"), None),
        P("scene"),
        P(("scene", "tile", "band"), None, None),
    )
    out_specs = (P(("scene", "tile", "band"), "half", None), P(("scene", "tile", "band"), None))
    return jax.shard_map(local, mesh=mesh, in_specs=in_specs, out_specs=out_specs, check_vma=False)
```
